256 devices in a mesh: seq: 32 (over z, y_lo, core), grp: 8 (over x, y_hi).
Axes of the slice: x: 4, y: 4 (y_hi: 2, y_lo: 2; y = y_hi * 2 + y_lo), z: 8, core: 2. Of those that a mesh axis runs over, the one named last changes fastest.
Arguments:
- prompt_tokens: bfloat16 [32768, 2048], P('seq'), may hold values from -6 to 6
- response_tokens: bfloat16 [8, 32, 256, 2048], P('grp', 'seq'), may hold values from -6 to 6
- w_query: bfloat16 [2048, 1024], P('seq', 'grp'), may hold values from -0.125 to 0.125
- w_key: bfloat16 [2048, 1024], P('seq', 'grp'), may hold values from -0.125 to 0.125
- w_value: bfloat16 [2048, 2048], P('seq', 'grp'), may hold values from -0.125 to 0.125
- w_decay: bfloat16 [2048, 16], P('seq', 'grp'), may hold values from -0.125 to 0.125
- w_beta: bfloat16 [2048, 16], P('seq', 'grp'), may hold values from -0.125 to 0.125
- decay_rate: float32 [16], replicated, may hold values from 0 to 0.06
- beta_shift: float32 [16], replicated, may hold values from -9 to 1
- out_gain: float32 [128], replicated, may hold values from 0.25 to 1.75
- resp_lengths: int32 [8, 32], P('grp', 'seq'), may hold values from 1 to 256, 4096 in all within a row
Outputs:
- prompt_output: bfloat16 [32768, 2048], P('seq', 'grp')
- response_output: bfloat16 [8, 32, 256, 2048], P('grp', 'seq')
The draws below stay inside these ranges and needn't reach their ends.
Inputs may be any that keep to these rules, and one draw needn't show every extreme that they name: `resp_lengths`: in every group one response has exactly 256 tokens, and a group's lengths sum to 4096.
All inputs are finite; a program needn't handle non-finite values.
Results may differ from the reference program's by a relative error of at most 0.0062.
Values may be sent and summed in bfloat16 or wider, within the bound.
No kernel may reach another device: no remote copies, remote signals or barrier semaphores. Data moves between devices by JAX's collectives and lax.ppermute only.
A program may use at most 128 MiB of HBM per device.

```python
import math
import jax
import jax.numpy as jnp
import numpy as np
from jax import lax

D = 2048
DK = 128
DV = 128
HK = 8
HV = 16
RLEN = 256
P_DEV = 1024
P_TOKENS = 32768
N_SEQ = 32
N_GRP = 8


def head_kinds(key):
    pick = jax.random.uniform(jax.random.fold_in(key, 71), (HV,), jnp.float32)
    first = jax.random.uniform(jax.random.fold_in(key, 72), (HV,), jnp.float32)
    second = jax.random.uniform(jax.random.fold_in(key, 73), (HV,), jnp.float32)
    slow = pick < 0.5
    return (slow, first, second)


def draw_decay_rate(key, part):
    slow, first, second = head_kinds(key)
    chain = P_DEV * N_SEQ
    slow_rate = 0.1 / chain * 5.0 ** first
    fast_rate = 0.025 * 2.4 ** second
    return jnp.where(slow, slow_rate, fast_rate).astype(jnp.float32)


def draw_beta_shift(key, part):
    slow, first, second = head_kinds(key)
    chain = P_DEV * N_SEQ
    slow_shift = jnp.log(DK / chain) - 1.0 + (second - 0.5)
    fast_shift = 2.0 * first - 1.0
    return jnp.where(slow, slow_shift, fast_shift).astype(jnp.float32)


def levels(key, shape, shards, least, top_value):
    def one(dim, blocks):
        steps = jax.random.uniform(jax.random.fold_in(jax.random.fold_in(key, 6), dim), (blocks,), jnp.float32, least / len(shards), top_value / len(shards))
        return jnp.repeat(jnp.exp(steps), shape[dim] // blocks).reshape((-1,) + (1,) * (len(shape) - dim - 1))

    factor_of = one(*shards[0])
    for cut in shards[1:]:
        factor_of = factor_of * one(*cut)
    return factor_of


def length_profile(number_of, total, reach, skew):
    loads = [(1 << 20) // math.isqrt(standing ** skew) + 1 for standing in range(2, number_of + 1)]
    spare, holding = total - reach - (number_of - 1), [1] * (number_of - 1)
    while spare > 0:
        free = [i for i in range(number_of - 1) if holding[i] < reach]
        pool, left = sum([loads[i] for i in free]), spare
        for i in free:
            more = min(reach - holding[i], max(1, left * loads[i] // pool), spare)
            holding[i] = holding[i] + more
            spare = spare - more
    return np.array([reach] + holding)


def uneven_parts(rng, count, total, most, lean):
    if count == 2:
        one = jax.random.randint(rng, (), max(1, total - most), min(most, total - 1) + 1)
        return jnp.stack([one, total - one])
    sizes = jnp.asarray(length_profile(count, total, most, lean), jnp.int32)
    twos = (count - 1) // 2
    giver, sink = sizes[1:1 + 2 * twos:2], sizes[2:2 + 2 * twos:2]
    slack = jnp.minimum(giver - 1, most - sink)
    passed = jax.random.randint(jax.random.fold_in(rng, 1), (twos,), 0, 1 << 20) % (slack + 1)
    sizes = sizes.at[1:1 + 2 * twos:2].set(giver - passed).at[2:2 + 2 * twos:2].set(sink + passed)
    return sizes[jax.random.permutation(jax.random.fold_in(rng, 2), count)]


def noise(stream_key, dims, spread, most, cuts=(), kind=jnp.bfloat16):
    factor_of = levels(stream_key, dims, cuts, -0.22, 0.18) if cuts else 1.0
    entries = jax.random.normal(stream_key, dims, jnp.float32) * spread * factor_of
    return jnp.minimum(jnp.maximum(entries, -most), most).astype(kind)


def setup_inputs(seed: int = 0) -> dict:
    streams_of = jax.random.split(jax.random.key(seed), 12)
    return {
        "prompt_tokens": noise(streams_of[0], (P_TOKENS, D), 1.0, 6.0, ((0, 32),)),
        "response_tokens": noise(streams_of[1], (N_GRP, N_SEQ, RLEN, D), 1.0, 6.0, ((0, 8), (1, 32))),
        "w_query": noise(streams_of[2], (D, HK * DK), D ** -0.5, 0.125, ((0, 32), (1, 8))),
        "w_key": noise(streams_of[3], (D, HK * DK), D ** -0.5, 0.125, ((0, 32), (1, 8))),
        "w_value": noise(streams_of[4], (D, HV * DV), D ** -0.5, 0.125, ((0, 32), (1, 8))),
        "w_decay": noise(streams_of[5], (D, HV), D ** -0.5, 0.125, ((0, 32), (1, 8))),
        "w_beta": noise(streams_of[6], (D, HV), D ** -0.5, 0.125, ((0, 32), (1, 8))),
        "decay_rate": draw_decay_rate(jax.random.fold_in(streams_of[11], 71), 0),
        "beta_shift": draw_beta_shift(jax.random.fold_in(streams_of[11], 71), 0),
        "out_gain": jnp.clip(1.0 + 0.15 * jax.random.normal(streams_of[9], (DV,), jnp.float32), 0.25, 1.75),
        "resp_lengths": jax.vmap(lambda own: uneven_parts(own, N_SEQ, N_SEQ * RLEN // 2, RLEN, 2))(jax.random.split(streams_of[10], N_GRP)).reshape((N_GRP, N_SEQ)).astype(jnp.int32),
    }


def make_heads(x, weights, rate, shift):
    raw = [jnp.dot(x, w, preferred_element_type=jnp.float32) for w in weights]
    count = x.shape[0]
    key_heads = raw[0].shape[1] // DK
    value_heads = raw[3].shape[1]
    repeat = value_heads // key_heads
    query_rows = raw[0].reshape(count, key_heads, DK)
    keys = raw[1].reshape(count, key_heads, DK)
    query_rows = query_rows * lax.rsqrt(lax.optimization_barrier(jnp.sum(query_rows * query_rows, axis=-1, keepdims=True)) + 1e-06) * DK ** (-0.5)
    keys = keys * lax.rsqrt(lax.optimization_barrier(jnp.sum(keys * keys, axis=-1, keepdims=True)) + 1e-06)
    query_rows = jnp.repeat(query_rows.astype(jnp.bfloat16), repeat, axis=1)
    keys = jnp.repeat(keys.astype(jnp.bfloat16), repeat, axis=1)
    values = raw[2].reshape(count, value_heads, raw[2].shape[1] // value_heads).astype(jnp.bfloat16)
    log_decay = -rate * jax.nn.softplus(raw[3])
    beta = jax.nn.sigmoid(raw[4] + shift)
    return (query_rows, keys, values, log_decay, beta)

def finish(layer_output, gain):
    normed = layer_output * lax.rsqrt(lax.optimization_barrier(jnp.mean(layer_output * layer_output, axis=-1, keepdims=True)) + 1e-06) * gain
    return normed.reshape(normed.shape[:-2] + (normed.shape[-2] * normed.shape[-1],)).astype(jnp.bfloat16)

def recur(query_rows, keys, values, log_decay, beta, state_matrix):
    highest_level = lax.Precision.HIGHEST

    def advance(state_matrix, inputs):
        query_current, key_current, v_now, g_now, b_now = inputs
        query_current = query_current.astype(jnp.float32)
        key_current = key_current.astype(jnp.float32)
        v_now = v_now.astype(jnp.float32)
        running_along = jnp.einsum('...yt,...ytl->...yl', key_current, state_matrix, precision=highest_level)
        scaled = b_now[..., None, None] * key_current[..., :, None]
        kept = state_matrix - scaled * running_along[..., None, :]
        state_matrix = jnp.exp(g_now)[..., None, None] * kept + scaled * v_now[..., None, :]
        layer_output = jnp.einsum('...wog,...wo->...wg', state_matrix, query_current, precision=highest_level)
        return (state_matrix, layer_output)
    return lax.scan(advance, state_matrix, (query_rows, keys, values, log_decay, beta))

def reference(prompt_tokens, response_tokens, w_query, w_key, w_value, w_decay, w_beta, decay_rate, beta_shift, out_gain, resp_lengths):
    weights = (w_query, w_key, w_value, w_decay, w_beta)
    query_rows, keys, values, log_decay, beta = make_heads(prompt_tokens, weights, decay_rate, beta_shift)
    start = jnp.zeros((HV, DK, DV), jnp.float32)
    end_state, prompt_out = recur(query_rows, keys, values, log_decay, beta, start)
    prompt_output = finish(prompt_out, out_gain)
    count = N_GRP * N_SEQ
    flat = response_tokens.reshape(count * RLEN, D)
    parts = make_heads(flat, weights, decay_rate, beta_shift)
    arranged = tuple((jnp.swapaxes(p.reshape((count, RLEN) + p.shape[1:]), 0, 1) for p in parts))
    init = jnp.broadcast_to(end_state, (count, HV, DK, DV))
    final_unused, outs = recur(arranged[0], arranged[1], arranged[2], arranged[3], arranged[4], init)
    outs = jnp.swapaxes(outs, 0, 1)
    finished = finish(outs, out_gain)
    positions = jnp.arange(RLEN, dtype=jnp.int32)
    live = positions[None, :] < resp_lengths.reshape(count)[:, None]
    masked = jnp.where(live[..., None], finished, jnp.zeros_like(finished))
    return (prompt_output, masked.reshape(N_GRP, N_SEQ, RLEN, HV * DV))
```

```python
import jax, jax.numpy as jnp
from jax import lax
from jax.sharding import Mesh
from jax.sharding import PartitionSpec as P
from jax.experimental import pallas as pl
from jax.experimental.pallas import tpu as pltpu

F32 = jnp.float32
BF16 = jnp.bfloat16
DK = 128
SPAN = 128
DEPTH = 2048
WIDTH = 8
VMEM = pl.BlockSpec(memory_space=pltpu.VMEM)
SMEM = pl.BlockSpec(memory_space=pltpu.SMEM)


def mm(a, b, ca=1, cb=0):
    return lax.dot_general(a, b, (((ca,), (cb,)), ((), ())), preferred_element_type=F32)


def halves(a):
    high = a.astype(BF16)
    return high, (a - high.astype(F32)).astype(BF16)


def mm_wide(a, b):
    a_high, a_low = halves(a)
    b_high, b_low = halves(b)
    return mm(a_high, b_high) + (mm(a_high, b_low) + mm(a_low, b_high))


def mm_low(a, b):
    return mm(a.astype(BF16), b.astype(BF16))


def mm_state(a, state):
    high, low = halves(state)
    return mm(a, high) + mm(a, low)


def unit_row(raw, scale):
    return (raw * (lax.rsqrt(jnp.sum(raw * raw, axis=-1, keepdims=True) + 1e-06) * scale)).astype(BF16)


def solve_units(lowers, row, column):
    ident = jnp.where(row == column, 1.0, 0.0).astype(F32)
    inside = (row // 8) == (column // 8)
    bases = [jnp.where(inside, lower, 0.0) for lower in lowers]
    squares = [mm_wide(base, base) for base in bases]
    fourths = [mm_wide(square, square) for square in squares]
    results = [ident - base for base in bases]
    results = [r + mm_wide(r, square) for r, square in zip(results, squares)]
    results = [r + mm_wide(r, fourth) for r, fourth in zip(results, fourths)]
    size = 8
    while size < SPAN:
        across = ((row // (2 * size)) == (column // (2 * size))) & (
            (row // size) != (column // size)
        )
        joined = [jnp.where(across, lower, 0.0).astype(BF16) for lower in lowers]
        rounded = [r.astype(BF16) for r in results]
        halfway = [mm(r, a).astype(BF16) for r, a in zip(rounded, joined)]
        results = [r - mm(h, b) for r, h, b in zip(results, halfway, rounded)]
        size *= 2
    return results


def make_body(chain, parts):
    def body(scalar_ref, gate_ref, x_refs, own_ref, other_ref, out_ref, map_ref,
             wqk_ref, wv_ref, wab_ref, q_ref, k_ref, v_ref, g_ref, b_ref,
             u_ref, lhs_ref, lhs2_ref, last_ref):
        second = scalar_ref[0]
        for block in range(16):
            rows = pl.ds(block * 128, 128)
            mine = own_ref[block]
            others = other_ref[block]
            first_half = jnp.where(second == 0, mine, others)
            second_half = jnp.where(second == 0, others, mine)
            wqk_ref[rows, :] = first_half[:128]
            wv_ref[rows, :] = second_half[:128]
            tall = jnp.concatenate(
                [first_half[128:136, :128].astype(F32), jnp.zeros((120, 128), F32)], axis=0
            )
            wab_ref[rows, :] = tall.T.astype(BF16)
        count = sum(x_ref.shape[0] for x_ref in x_refs)
        tril = jnp.where(
            lax.broadcasted_iota(jnp.int32, (SPAN, SPAN), 0)
            >= lax.broadcasted_iota(jnp.int32, (SPAN, SPAN), 1),
            1.0,
            0.0,
        ).astype(BF16)
        lane = lax.broadcasted_iota(jnp.int32, (1, 128), 1)
        rate = jnp.where(lane == 0, gate_ref[0], jnp.where(lane == 1, gate_ref[1], 0.0))
        shift = jnp.where(lane == 2, gate_ref[2], jnp.where(lane == 3, gate_ref[3], 0.0))
        for part in range(count // 256):
            rows = pl.ds(part * 256, 256)
            x = x_refs[part][...] if len(x_refs) > 1 else x_refs[0][rows, :]
            qk = mm(x, wqk_ref[...])
            q_ref[rows, :] = unit_row(qk[:, :128], DK ** (-0.5))
            k_ref[rows, :] = unit_row(qk[:, 128:], 1.0)
            v_ref[rows, :] = mm(x, wv_ref[...]).astype(BF16)
            ab = mm(x, wab_ref[...])
            g_ref[rows, :] = -rate * jnp.logaddexp(ab, 0.0)
            b_ref[rows, :] = 1.0 / (1.0 + jnp.exp(-(ab + shift)))
        row = lax.broadcasted_iota(jnp.int32, (SPAN, SPAN), 0)
        column = lax.broadcasted_iota(jnp.int32, (SPAN, SPAN), 1)
        spans = count // SPAN

        def prepare(index, carry):
            chains = [(sub, head) for sub in range(WIDTH) for head in range(2)]
            spans_now = [index * WIDTH + sub for sub in range(WIDTH)]
            rows = [pl.ds(pl.multiple_of(span * SPAN, SPAN), SPAN) for span in spans_now]
            q = [q_ref[r, :] for r in rows]
            k = [k_ref[r, :] for r in rows]
            beta = [b_ref[r, :] for r in rows]
            pieces = []
            for r in rows:
                g = g_ref[r, :]
                g_high, g_low = halves(g)
                pieces.append(
                    (g_high, g_low, (g - g_high.astype(F32) - g_low.astype(F32)).astype(BF16))
                )
            cumul = [mm(tril, p[0]) + (mm(tril, p[1]) + mm(tril, p[2])) for p in pieces]
            cumul_t = [c.T for c in cumul]
            kk = [mm(a, a, 1, 1) for a in k]
            qk = [mm(a, b, 1, 1) for a, b in zip(q, k)]
            col = [jnp.broadcast_to(cumul[s][:, h:h + 1], (SPAN, SPAN)) for s, h in chains]
            decay = [
                jnp.where(
                    row >= column, jnp.exp(jnp.minimum(c - cumul_t[s][h:h + 1, :], 0.0)), 0.0
                )
                for c, (s, h) in zip(col, chains)
            ]
            strength = [
                jnp.broadcast_to(beta[s][:, 2 + h:3 + h], (SPAN, SPAN)) for s, h in chains
            ]
            lowers = [
                jnp.where(row > column, b * d * kk[s], 0.0)
                for b, d, (s, h) in zip(strength, decay, chains)
            ]
            inverses = solve_units(lowers, row, column)
            solved = []
            for n, (s, h) in enumerate(chains):
                v = v_ref[rows[s], h * 128:(h + 1) * 128].astype(F32)
                rhs = jnp.concatenate(
                    [strength[n] * v, strength[n] * jnp.exp(col[n]) * k[s].astype(F32)], axis=1
                )
                solved.append(mm_low(inverses[n], rhs))
            for n, (s, h) in enumerate(chains):
                both = pl.ds(pl.multiple_of(spans_now[s] * 2 * SPAN, 2 * SPAN), 2 * SPAN)
                end = cumul[s][SPAN - 1:SPAN, h:h + 1]
                tail = jnp.exp(jnp.broadcast_to(end, (SPAN, SPAN)) - col[n]) * k[s].astype(F32)
                u_ref[h, rows[s], :] = solved[n][:, :128]
                lhs_ref[h, both, :] = jnp.concatenate(
                    [solved[n][:, 128:], jnp.exp(col[n]) * q[s].astype(F32)], axis=0
                ).astype(BF16)
                lhs2_ref[h, both, :] = jnp.concatenate(
                    [decay[n] * qk[s], tail.T], axis=0
                ).astype(BF16)
                last_ref[h, pl.ds(spans_now[s], 1), :] = jnp.broadcast_to(jnp.exp(end), (1, 128))
            return carry

        lax.fori_loop(0, spans // WIDTH, prepare, 0)
        ident = jnp.where(row == column, 1.0, 0.0).astype(F32)
        start = jnp.concatenate([jnp.zeros((128, 128), F32), ident], axis=1)
        lines = [(group, head) for group in range(spans // chain) for head in range(2)]
        states = [start for unused in lines]
        for step in range(chain):
            at = [group * chain + step for group, head in lines]
            reads = [
                mm_state(lhs_ref[head, pl.ds(span * 2 * SPAN, 2 * SPAN), :], state)
                for span, (group, head), state in zip(at, lines, states)
            ]
            deltas = [
                jnp.concatenate(
                    [u_ref[head, pl.ds(span * SPAN, SPAN), :] - r[:128, :128], -r[:128, 128:]],
                    axis=1,
                ).astype(BF16)
                for span, (group, head), r in zip(at, lines, reads)
            ]
            writes = [
                mm(lhs2_ref[head, pl.ds(span * 2 * SPAN, 2 * SPAN), :], delta)
                for span, (group, head), delta in zip(at, lines, deltas)
            ]
            lasts = [last_ref[head, pl.ds(span, 1), :] for span, (group, head) in zip(at, lines)]
            for span, (group, head), r, w in zip(at, lines, reads, writes):
                out_ref[head, pl.ds(span * SPAN, SPAN), :] = r[128:] + w[:128]
            states = [
                jnp.concatenate([last, last], axis=1) * state + w[128:]
                for last, state, w in zip(lasts, states, writes)
            ]
        if map_ref is not None:
            for head in range(2):
                map_ref[head] = states[head]

    def entry(scalar_ref, gate_ref, *refs):
        x_refs, refs = refs[:parts], refs[parts:]
        own_ref, other_ref, out_ref = refs[:3]
        if parts == 1:
            body(scalar_ref, gate_ref, x_refs, own_ref, other_ref, out_ref, refs[3], *refs[4:])
        else:
            body(scalar_ref, gate_ref, x_refs, own_ref, other_ref, out_ref, None, *refs[3:])

    return entry


def delta_rule(second, gates, tokens, own, other, chain):
    count = sum(x.shape[0] for x in tokens)
    outs = [jax.ShapeDtypeStruct((2, count, 256), F32)]
    if len(tokens) == 1:
        outs.append(jax.ShapeDtypeStruct((2, 128, 256), F32))
    spans = count // SPAN
    return pl.pallas_call(
        make_body(chain, len(tokens)),
        out_shape=tuple(outs),
        in_specs=[SMEM, SMEM] + [VMEM] * (len(tokens) + 2),
        out_specs=tuple(VMEM for unused in outs),
        scratch_shapes=[
            pltpu.VMEM((DEPTH, 256), BF16),
            pltpu.VMEM((DEPTH, 256), BF16),
            pltpu.VMEM((DEPTH, 128), BF16),
            pltpu.VMEM((count, 128), BF16),
            pltpu.VMEM((count, 128), BF16),
            pltpu.VMEM((count, 256), BF16),
            pltpu.VMEM((count, 128), F32),
            pltpu.VMEM((count, 128), F32),
            pltpu.VMEM((2, count, 128), F32),
            pltpu.VMEM((2, 2 * count, 128), BF16),
            pltpu.VMEM((2, 2 * count, 128), BF16),
            pltpu.VMEM((2, max(spans, 8), 128), F32),
        ],
        cost_estimate=pl.CostEstimate(flops=2 * count * 2048 * 640 + 16 * 60 * 2 * 128**3, transcendentals=count * 1024, bytes_accessed=8 << 20),
        compiler_params=pltpu.CompilerParams(vmem_limit_bytes=48 << 20),
    )(second, gates, *tokens, own, other)


def call(body, outs, operands, scratch=(), flops=1 << 24):
    return pl.pallas_call(
        body,
        out_shape=tuple(outs),
        in_specs=[SMEM if a.ndim == 1 else VMEM for a in operands],
        out_specs=tuple(VMEM for unused in outs),
        scratch_shapes=list(scratch),
        cost_estimate=pl.CostEstimate(flops=flops, transcendentals=0, bytes_accessed=1 << 20),
        compiler_params=pltpu.CompilerParams(vmem_limit_bytes=48 << 20),
    )(*operands)


def identity():
    row = lax.broadcasted_iota(jnp.int32, (128, 128), 0)
    column = lax.broadcasted_iota(jnp.int32, (128, 128), 1)
    return jnp.where(row == column, 1.0, 0.0).astype(F32)


def join_maps(second_core, kept, got):
    def body(second_ref, kept_ref, got_ref, first_ref, chip_ref):
        second = second_ref[0]
        mine = kept_ref[...]
        others = got_ref[...]
        first = jnp.where(second == 0, mine, others)
        last = jnp.where(second == 0, others, mine)
        first_ref[...] = first
        joined = mm_wide(last[:, 128:], first)
        chip_ref[...] = jnp.concatenate(
            [joined[:, :128] + last[:, :128], joined[:, 128:] - identity()], axis=1
        ).astype(BF16)

    shape = (128, 256)
    return call(
        body,
        [jax.ShapeDtypeStruct(shape, F32), jax.ShapeDtypeStruct(shape, BF16)],
        (second_core, kept, got),
    )


def join_chips(upper, kept, got):
    def body(upper_ref, kept_ref, got_ref, first_ref, pair_ref):
        mine = kept_ref[...]
        others = got_ref[...]
        first = jnp.where(upper_ref[0] == 0, mine, others)
        last = jnp.where(upper_ref[0] == 0, others, mine)
        first_ref[...] = first
        joined = mm(last[:, 128:], first) + first.astype(F32) + last.astype(F32)
        pair_ref[...] = joined.astype(BF16)

    shape = jax.ShapeDtypeStruct((128, 256), BF16)
    return call(body, [shape, shape], (upper, kept, got))


def run_prefix(place, pieces, first_chip, first, after):
    pairs = len(pieces)

    def body(place_ref, *refs):
        piece_refs = refs[:pairs]
        chip_ref, first_ref, unused, start_ref, end_ref, sorted_ref = refs[pairs:]
        me = place_ref[0]
        for shift in range(pairs):
            sorted_ref[lax.rem(me + pairs - shift, pairs)] = piece_refs[shift][...]
        state = jnp.zeros((128, 128), F32)
        for pair in range(pairs):
            @pl.when(me == pair)
            def store_start(state=state):
                start_ref[0] = state

            piece = sorted_ref[pair]
            state = state + mm_state(piece[:, 128:], state) + piece[:, :128].astype(F32)
        end_ref[...] = state
        chip = chip_ref[...]
        begin = start_ref[0]
        moved = begin + mm_state(chip[:, 128:], begin) + chip[:, :128].astype(F32)
        begin = jnp.where(place_ref[1] == 0, begin, moved)
        start_ref[0] = begin
        first = first_ref[...]
        start_ref[1] = mm_wide(first[:, 128:], begin) + first[:, :128]

    return pl.pallas_call(
        body,
        out_shape=(
            jax.ShapeDtypeStruct((2, 128, 128), F32),
            jax.ShapeDtypeStruct((128, 128), F32),
        ),
        in_specs=[SMEM] + [VMEM] * (pairs + 2) + [pl.BlockSpec(memory_space=pl.ANY)],
        out_specs=(VMEM, VMEM),
        scratch_shapes=[pltpu.VMEM((pairs, 128, 256), BF16)],
        cost_estimate=pl.CostEstimate(flops=1 << 27, transcendentals=0, bytes_accessed=1 << 20),
    )(place, *pieces, first_chip, first, after)


def normed(local, lifted, state, gain):
    total = local + mm_wide(lifted, state)
    mean = jnp.mean(total * total, axis=-1, keepdims=True)
    return (total * lax.rsqrt(mean + 1e-06) * gain).astype(BF16)


def finish_prompt(outs, starts, gain):
    def body(outs_ref, starts_ref, gain_ref, result_ref):
        for head in range(2):
            for part in range(outs.shape[1] // 256):
                rows = pl.ds(part * 256, 256)
                both = outs_ref[head, rows, :]
                result_ref[rows, head * 128:(head + 1) * 128] = normed(
                    both[:, :128], both[:, 128:], starts_ref[head], gain_ref[...]
                )

    return call(
        body, [jax.ShapeDtypeStruct((outs.shape[1], 256), BF16)], (outs, starts, gain), (), 1 << 28
    )[0]


def finish_responses(flip, outs, outs_partner, ends, ends_partner, gain):
    parts = outs.shape[1] // 256

    def body(flip_ref, outs_ref, partner_ref, ends_ref, ends_partner_ref, gain_ref, *result_refs):
        for side, (source, states) in enumerate(
            ((outs_ref, ends_ref), (partner_ref, ends_partner_ref))
        ):
            base = (flip_ref[0] if side == 0 else 1 - flip_ref[0]) * 256
            for head in range(2):
                lanes = pl.ds(pl.multiple_of(base + head * 128, 128), 128)
                for part in range(parts):
                    both = source[head, pl.ds(part * 256, 256), :]
                    result_refs[part][:, lanes] = normed(
                        both[:, :128], both[:, 128:], states[head], gain_ref[...]
                    )

    return call(
        body,
        [jax.ShapeDtypeStruct((256, 512), BF16)] * parts,
        (flip, outs, outs_partner, ends, ends_partner, gain),
        (),
        1 << 29,
    )


def assemble(numbers, blocks):
    parts = len(blocks)

    def body(number_ref, *refs):
        result_ref = refs[parts]
        row = lax.broadcasted_iota(jnp.int32, (256, 512), 0)
        live = row < number_ref[1]
        for shift in range(parts):
            base = lax.rem(number_ref[0] + shift, parts) * 512
            block = refs[shift][...].astype(F32)
            result_ref[:, pl.ds(pl.multiple_of(base, 512), 512)] = jnp.where(
                live, block, 0.0
            ).astype(BF16)

    return call(body, [jax.ShapeDtypeStruct((256, 512 * parts), BF16)], (numbers, *blocks))[0]


def swap(array, axis):
    return lax.ppermute(array, axis, [(0, 1), (1, 0)])


def turn(array, axis, count, shift):
    return lax.ppermute(array, axis, [(i, (i + shift) % count) for i in range(count)])


CHIP = ("z", "y_lo")


def shards(
    prompt_tokens,
    response_tokens,
    w_query,
    w_key,
    w_value,
    w_decay,
    w_beta,
    decay_rate,
    beta_shift,
    out_gain,
    resp_lengths,
):
    core = lax.axis_index("core")
    along = lax.axis_index("x")
    side = lax.axis_index("y_hi")
    layer = lax.axis_index("z")
    upper = lax.axis_index("y_lo")
    layers = lax.axis_size("z")
    chips = lax.axis_size(CHIP)
    wide = lax.axis_size("x")
    tokens = response_tokens.reshape(response_tokens.shape[2:])
    token_parts = [tokens] + [turn(tokens, "x", wide, s) for s in range(1, wide)]

    rows = w_query.shape[0]
    gates_t = jnp.pad(jnp.concatenate([w_decay, w_beta], axis=1).T, ((0, 4), (0, 256 - rows)))
    pack_qk = jnp.concatenate([jnp.concatenate([w_query, w_key], axis=1), gates_t], axis=0)
    pack_v = jnp.concatenate([w_value, gates_t], axis=0)
    got = swap(jnp.where(core == 0, pack_v, pack_qk), "core")
    kept = jnp.where(core == 0, pack_qk, pack_v)
    low = jnp.where(core == 0, kept, got)
    high = jnp.where(core == 0, got, kept)
    mixed = jnp.concatenate(
        [low[rows:, :rows], high[rows:, :rows], jnp.zeros((8, 256 - 2 * rows), BF16)], axis=1
    )
    block = jnp.concatenate([low[:rows], high[:rows], mixed], axis=0)
    own = lax.all_to_all(
        jnp.broadcast_to(block[None], (chips,) + block.shape), CHIP, 0, 0, tiled=True
    )
    other = swap(own, "core")
    partner_own = swap(own, "y_hi")
    partner_other = swap(partner_own, "core")

    def gates_of(group):
        return jnp.concatenate(
            [
                lax.dynamic_slice_in_dim(decay_rate, group * 2, 2),
                lax.dynamic_slice_in_dim(beta_shift, group * 2, 2),
            ]
        )

    core_number = core.reshape(1)
    gain = out_gain.reshape(1, 128)
    group = along * 2 + side
    outs, maps = delta_rule(core_number, gates_of(group), (prompt_tokens,), own, other, 8)
    mine = lax.dynamic_index_in_dim(maps, core, 0, keepdims=False)
    theirs = lax.dynamic_index_in_dim(maps, 1 - core, 0, keepdims=False)
    first, chip_map = join_maps(core_number, mine, swap(theirs, "core"))
    first_chip, pair_map = join_chips(upper.reshape(1), chip_map, swap(chip_map, "y_lo"))
    pieces = [pair_map] + [turn(pair_map, "z", layers, s) for s in range(1, layers)]
    (resp_outs,) = delta_rule(core_number, gates_of(group), token_parts, own, other, 2)
    starts, end = run_prefix(jnp.stack([layer, upper]), pieces, first_chip, first, resp_outs)
    (resp_partner,) = delta_rule(
        core_number, gates_of(along * 2 + 1 - side), token_parts, partner_own, partner_other, 2
    )
    start_mine = lax.dynamic_index_in_dim(starts, core, 0, keepdims=False)
    start_theirs = lax.dynamic_index_in_dim(starts, 1 - core, 0, keepdims=False)
    sent = swap(jnp.stack([start_theirs, end]), "core")
    start_heads = jnp.stack(
        [jnp.where(core == 0, start_mine, sent[0]), jnp.where(core == 0, sent[0], start_mine)]
    )
    end_heads = jnp.stack([jnp.where(core == 0, end, sent[1]), jnp.where(core == 0, sent[1], end)])
    end_partner = swap(end_heads, "y_hi")
    parts = finish_responses(side.reshape(1), resp_outs, resp_partner, end_heads, end_partner, gain)
    blocks = [parts[0]] + [turn(parts[s], "x", wide, -s) for s in range(1, wide)]
    prompt_output = finish_prompt(outs, start_heads, gain)
    numbers = jnp.stack([along, resp_lengths.reshape(())])
    result = assemble(numbers, blocks)
    return (prompt_output, result.reshape((1, 1) + result.shape))


def solution(mesh):
    devices = mesh.devices.reshape(mesh.shape["seq"] // 4, 2, 2, mesh.shape["grp"] // 2, 2)
    torus = Mesh(devices, ("z", "y_lo", "core", "x", "y_hi"))
    seq = ("z", "y_lo", "core")
    grp = ("x", "y_hi")
    weight = P(seq, grp)
    placed = (P(seq, None), P(grp, seq, None, None)) + (weight,) * 5 + (P(),) * 3 + (P(grp, seq),)
    return jax.shard_map(
        shards,
        mesh=torus,
        in_specs=placed,
        out_specs=(P(seq, grp), P(grp, seq, None, None)),
        check_vma=False,
    )
```

```python
import jax, jax.numpy as jnp
from jax import lax
from jax.sharding import Mesh
from jax.sharding import PartitionSpec as P
from jax.experimental import pallas as pl
from jax.experimental.pallas import tpu as pltpu


F32 = jnp.float32
BF16 = jnp.bfloat16
DK = 128
SPAN = 128
DEPTH = 2048
WIDTH = 8
ORDER = (0, 7, 1, 6, 2, 5, 3, 4)
VMEM = pl.BlockSpec(memory_space=pltpu.VMEM)
SMEM = pl.BlockSpec(memory_space=pltpu.SMEM)


def mm(a, b, ca=1, cb=0):
    return lax.dot_general(a, b, (((ca,), (cb,)), ((), ())), preferred_element_type=F32)


def halves(a):
    high = a.astype(BF16)
    return high, (a - high.astype(F32)).astype(BF16)


def mm_wide(a, b):
    a_high, a_low = halves(a)
    b_high, b_low = halves(b)
    a_both = jnp.concatenate([a_high, a_low], axis=1)
    return mm(a_both, jnp.concatenate([b_high, b_high], axis=0)) + mm(a_high, b_low)


def mm_low(a, b):
    return mm(a.astype(BF16), b.astype(BF16))


def mm_state(a, state):
    return mm(jnp.concatenate([a, a], axis=1), jnp.concatenate(halves(state), axis=0))


def unit_row(raw, scale):
    return (raw * (lax.rsqrt(jnp.sum(raw * raw, axis=-1, keepdims=True) + 1e-06) * scale)).astype(BF16)


def solve_units(lowers, row, column):
    ident = jnp.where(row == column, 1.0, 0.0).astype(F32)
    inside = (row // 8) == (column // 8)
    bases = [jnp.where(inside, lower, 0.0) for lower in lowers]
    squares = [mm_wide(base, base) for base in bases]
    fourths = [mm_wide(square, square) for square in squares]
    results = [ident - base for base in bases]
    results = [r + mm_wide(r, square) for r, square in zip(results, squares)]
    results = [r + mm_wide(r, fourth) for r, fourth in zip(results, fourths)]
    size = 8
    while size < SPAN:
        across = ((row // (2 * size)) == (column // (2 * size))) & (
            (row // size) != (column // size)
        )
        joined = [jnp.where(across, lower, 0.0).astype(BF16) for lower in lowers]
        rounded = [r.astype(BF16) for r in results]
        halfway = [mm(r, a).astype(BF16) for r, a in zip(rounded, joined)]
        results = [r - mm(h, b) for r, h, b in zip(results, halfway, rounded)]
        size *= 2
    return results


def make_body(chain, parts):
    def body(scalar_ref, gate_ref, x_refs, own_ref, other_ref, out_ref, map_ref, lent_ref,
             wqk_ref, wv_ref, wab_ref, q_ref, k_ref, v_ref, g_ref, b_ref,
             u_ref, lhs_ref, lhs2_ref, last_ref):
        second = scalar_ref[0]
        for block in range(16):
            place = lax.rem(scalar_ref[1] + ORDER[block // 2], 8) * 2 + block % 2
            rows = pl.ds(pl.multiple_of(place * 128, 128), 128)
            mine = own_ref[block // 2, block % 2]
            others = other_ref[block // 2, block % 2]
            first_half = jnp.where(second == 0, mine, others)
            second_half = jnp.where(second == 0, others, mine)
            wqk_ref[rows, :] = first_half[:128]
            wv_ref[rows, :] = second_half[:128]
            tall = jnp.concatenate(
                [first_half[128:136, :128].astype(F32), jnp.zeros((120, 128), F32)], axis=0
            )
            wab_ref[rows, :] = tall.T.astype(BF16)
        count = sum(x_ref.shape[0] for x_ref in x_refs)
        tril = jnp.where(
            lax.broadcasted_iota(jnp.int32, (SPAN, SPAN), 0)
            >= lax.broadcasted_iota(jnp.int32, (SPAN, SPAN), 1),
            1.0,
            0.0,
        ).astype(BF16)
        lane = lax.broadcasted_iota(jnp.int32, (1, 128), 1)
        rate = jnp.where(lane == 0, gate_ref[0], jnp.where(lane == 1, gate_ref[1], 0.0))
        shift = jnp.where(lane == 2, gate_ref[2], jnp.where(lane == 3, gate_ref[3], 0.0))
        for part in range(count // 256):
            rows = pl.ds(part * 256, 256)
            x = x_refs[part][...] if len(x_refs) > 1 else x_refs[0][rows, :]
            qk = mm(x, wqk_ref[...])
            q_ref[rows, :] = unit_row(qk[:, :128], DK ** (-0.5))
            k_ref[rows, :] = unit_row(qk[:, 128:], 1.0)
            v_ref[rows, :] = mm(x, wv_ref[...]).astype(BF16)
            ab = mm(x, wab_ref[...])
            g_ref[rows, :] = -rate * jnp.logaddexp(ab, 0.0)
            b_ref[rows, :] = 1.0 / (1.0 + jnp.exp(-(ab + shift)))
        row = lax.broadcasted_iota(jnp.int32, (SPAN, SPAN), 0)
        column = lax.broadcasted_iota(jnp.int32, (SPAN, SPAN), 1)
        spans = count // SPAN

        def prepare(index, carry):
            chains = [(sub, head) for sub in range(WIDTH) for head in range(2)]
            spans_now = [index * WIDTH + sub for sub in range(WIDTH)]
            rows = [pl.ds(pl.multiple_of(span * SPAN, SPAN), SPAN) for span in spans_now]
            q = [q_ref[r, :] for r in rows]
            k = [k_ref[r, :] for r in rows]
            beta = [b_ref[r, :] for r in rows]
            pieces = []
            for r in rows:
                g = g_ref[r, :]
                g_high, g_low = halves(g)
                pieces.append(
                    (g_high, g_low, (g - g_high.astype(F32) - g_low.astype(F32)).astype(BF16))
                )
            cumul = [
                mm(jnp.concatenate([tril, tril], axis=1), jnp.concatenate(p[:2], axis=0))
                + mm(tril, p[2])
                for p in pieces
            ]
            cumul_t = [c.T for c in cumul]
            kk = [mm(a, a, 1, 1) for a in k]
            qk = [mm(a, b, 1, 1) for a, b in zip(q, k)]
            col = [jnp.broadcast_to(cumul[s][:, h:h + 1], (SPAN, SPAN)) for s, h in chains]
            decay = [
                jnp.where(
                    row >= column, jnp.exp(jnp.minimum(c - cumul_t[s][h:h + 1, :], 0.0)), 0.0
                )
                for c, (s, h) in zip(col, chains)
            ]
            strength = [
                jnp.broadcast_to(beta[s][:, 2 + h:3 + h], (SPAN, SPAN)) for s, h in chains
            ]
            lowers = [
                jnp.where(row > column, b * d * kk[s], 0.0)
                for b, d, (s, h) in zip(strength, decay, chains)
            ]
            inverses = solve_units(lowers, row, column)
            solved = []
            for n, (s, h) in enumerate(chains):
                v = v_ref[rows[s], h * 128:(h + 1) * 128].astype(F32)
                rhs = jnp.concatenate(
                    [strength[n] * v, strength[n] * jnp.exp(col[n]) * k[s].astype(F32)], axis=1
                )
                solved.append(mm_low(inverses[n], rhs))
            for n, (s, h) in enumerate(chains):
                both = pl.ds(pl.multiple_of(spans_now[s] * 2 * SPAN, 2 * SPAN), 2 * SPAN)
                end = cumul[s][SPAN - 1:SPAN, h:h + 1]
                tail = jnp.exp(jnp.broadcast_to(end, (SPAN, SPAN)) - col[n]) * k[s].astype(F32)
                u_ref[h, rows[s], :] = solved[n][:, :128]
                lhs_ref[h, both, :] = jnp.concatenate(
                    [solved[n][:, 128:], jnp.exp(col[n]) * q[s].astype(F32)], axis=0
                ).astype(BF16)
                lhs2_ref[h, both, :] = jnp.concatenate(
                    [decay[n] * qk[s], tail.T], axis=0
                ).astype(BF16)
                last_ref[h, pl.ds(spans_now[s], 1), :] = jnp.broadcast_to(jnp.exp(end), (1, 128))
            return carry

        lax.fori_loop(0, spans // WIDTH, prepare, 0)
        ident = jnp.where(row == column, 1.0, 0.0).astype(F32)
        start = jnp.concatenate([jnp.zeros((128, 128), F32), ident], axis=1)
        lines = [(group, head) for group in range(spans // chain) for head in range(2)]
        states = [start for unused in lines]
        for step in range(chain):
            at = [group * chain + step for group, head in lines]
            reads = [
                mm_state(lhs_ref[head, pl.ds(span * 2 * SPAN, 2 * SPAN), :], state)
                for span, (group, head), state in zip(at, lines, states)
            ]
            deltas = [
                jnp.concatenate(
                    [u_ref[head, pl.ds(span * SPAN, SPAN), :] - r[:128, :128], -r[:128, 128:]],
                    axis=1,
                ).astype(BF16)
                for span, (group, head), r in zip(at, lines, reads)
            ]
            writes = [
                mm(lhs2_ref[head, pl.ds(span * 2 * SPAN, 2 * SPAN), :], delta)
                for span, (group, head), delta in zip(at, lines, deltas)
            ]
            lasts = [last_ref[head, pl.ds(span, 1), :] for span, (group, head) in zip(at, lines)]
            for span, (group, head), r, w in zip(at, lines, reads, writes):
                out_ref[head, pl.ds(span * SPAN, SPAN), :] = r[128:] + w[:128]
            states = [
                jnp.concatenate([last, last], axis=1) * state + w[128:]
                for last, state, w in zip(lasts, states, writes)
            ]
        if map_ref is not None:
            second_core = scalar_ref[0] == 1
            map_ref[...] = jnp.where(second_core, states[1], states[0])
            lent_ref[...] = jnp.where(second_core, states[0], states[1])

    def entry(scalar_ref, gate_ref, *refs):
        x_refs, refs = refs[:parts], refs[parts:]
        own_ref, other_ref, out_ref = refs[:3]
        if parts == 1:
            body(scalar_ref, gate_ref, x_refs, own_ref, other_ref, out_ref, *refs[3:])
        else:
            body(scalar_ref, gate_ref, x_refs, own_ref, other_ref, out_ref, None, None, *refs[3:])

    return entry


def delta_rule(second, gates, tokens, own, other, chain):
    count = sum(x.shape[0] for x in tokens)
    outs = [jax.ShapeDtypeStruct((2, count, 256), F32)]
    if len(tokens) == 1:
        outs += [jax.ShapeDtypeStruct((128, 256), F32)] * 2
    spans = count // SPAN
    return pl.pallas_call(
        make_body(chain, len(tokens)),
        out_shape=tuple(outs),
        in_specs=[SMEM, SMEM] + [VMEM] * (len(tokens) + 2),
        out_specs=tuple(VMEM for unused in outs),
        scratch_shapes=[
            pltpu.VMEM((DEPTH, 256), BF16),
            pltpu.VMEM((DEPTH, 256), BF16),
            pltpu.VMEM((DEPTH, 128), BF16),
            pltpu.VMEM((count, 128), BF16),
            pltpu.VMEM((count, 128), BF16),
            pltpu.VMEM((count, 256), BF16),
            pltpu.VMEM((count, 128), F32),
            pltpu.VMEM((count, 128), F32),
            pltpu.VMEM((2, count, 128), F32),
            pltpu.VMEM((2, 2 * count, 128), BF16),
            pltpu.VMEM((2, 2 * count, 128), BF16),
            pltpu.VMEM((2, max(spans, 8), 128), F32),
        ],
        cost_estimate=pl.CostEstimate(flops=2 * count * 2048 * 640 + 16 * 60 * 2 * 128**3, transcendentals=count * 1024, bytes_accessed=8 << 20),
        compiler_params=pltpu.CompilerParams(vmem_limit_bytes=48 << 20),
    )(second, gates, *tokens, own, other)


def call(body, outs, operands, scratch=(), flops=1 << 24):
    return pl.pallas_call(
        body,
        out_shape=tuple(outs),
        in_specs=[SMEM if a.ndim == 1 else VMEM for a in operands],
        out_specs=tuple(VMEM for unused in outs),
        scratch_shapes=list(scratch),
        cost_estimate=pl.CostEstimate(flops=flops, transcendentals=0, bytes_accessed=1 << 20),
        compiler_params=pltpu.CompilerParams(vmem_limit_bytes=48 << 20),
    )(*operands)


def identity():
    row = lax.broadcasted_iota(jnp.int32, (128, 128), 0)
    column = lax.broadcasted_iota(jnp.int32, (128, 128), 1)
    return jnp.where(row == column, 1.0, 0.0).astype(F32)


def join_maps(second_core, kept, got):
    def body(second_ref, kept_ref, got_ref, first_ref, chip_ref):
        second = second_ref[0]
        mine = kept_ref[...]
        others = got_ref[...]
        first = jnp.where(second == 0, mine, others)
        last = jnp.where(second == 0, others, mine)
        first_ref[...] = first
        joined = mm_wide(last[:, 128:], first)
        chip_ref[...] = jnp.concatenate(
            [joined[:, :128] + last[:, :128], joined[:, 128:] - identity()], axis=1
        ).astype(BF16)

    shape = (128, 256)
    return call(
        body,
        [jax.ShapeDtypeStruct(shape, F32), jax.ShapeDtypeStruct(shape, BF16)],
        (second_core, kept, got),
    )


def join_chips(upper, kept, got):
    def body(upper_ref, kept_ref, got_ref, first_ref, pair_ref):
        mine = kept_ref[...]
        others = got_ref[...]
        first = jnp.where(upper_ref[0] == 0, mine, others)
        last = jnp.where(upper_ref[0] == 0, others, mine)
        first_ref[...] = first
        joined = mm(last[:, 128:], first) + first.astype(F32) + last.astype(F32)
        pair_ref[...] = joined.astype(BF16)

    shape = jax.ShapeDtypeStruct((128, 256), BF16)
    return call(body, [shape, shape], (upper, kept, got))


def run_prefix(place, pieces, first_chip, first, after):
    pairs = len(pieces)

    def body(place_ref, *refs):
        piece_refs = refs[:pairs]
        chip_ref, first_ref, _, start_ref, send_ref, sorted_ref = refs[pairs:]
        me = place_ref[0]
        for shift in range(pairs):
            sorted_ref[lax.rem(me + pairs - shift, pairs)] = piece_refs[shift][...]
        state = jnp.zeros((128, 128), F32)
        for pair in range(pairs):
            @pl.when(me == pair)
            def store_start(state=state):
                start_ref[...] = state

            piece = sorted_ref[pair]
            state = state + mm_state(piece[:, 128:], state) + piece[:, :128].astype(F32)
        send_ref[1] = state
        chip = chip_ref[...]
        begin = start_ref[...]
        moved = begin + mm_state(chip[:, 128:], begin) + chip[:, :128].astype(F32)
        begin = jnp.where(place_ref[1] == 0, begin, moved)
        first = first_ref[...]
        later = mm_wide(first[:, 128:], begin) + first[:, :128]
        start_ref[...] = jnp.where(place_ref[2] == 0, begin, later)
        send_ref[0] = jnp.where(place_ref[2] == 0, later, begin)

    return pl.pallas_call(
        body,
        out_shape=(
            jax.ShapeDtypeStruct((128, 128), F32),
            jax.ShapeDtypeStruct((2, 128, 128), F32),
        ),
        in_specs=[SMEM] + [VMEM] * (pairs + 2) + [pl.BlockSpec(memory_space=pl.ANY)],
        out_specs=(VMEM, VMEM),
        scratch_shapes=[pltpu.VMEM((pairs, 128, 256), BF16)],
        cost_estimate=pl.CostEstimate(flops=1 << 27, transcendentals=0, bytes_accessed=1 << 20),
    )(place, *pieces, first_chip, first, after)


def normed(local, lifted, state, gain):
    total = local + mm_wide(lifted, state)
    mean = jnp.mean(total * total, axis=-1, keepdims=True)
    return (total * lax.rsqrt(mean + 1e-06) * gain).astype(BF16)


def finish_prompt(second_core, outs, start, got, gain):
    def body(second_ref, outs_ref, start_ref, got_ref, gain_ref, result_ref):
        mine = start_ref[...]
        others = got_ref[0]
        for head in range(2):
            state = jnp.where(second_ref[0] == head, mine, others)
            for part in range(outs.shape[1] // 256):
                rows = pl.ds(part * 256, 256)
                both = outs_ref[head, rows, :]
                result_ref[rows, head * 128:(head + 1) * 128] = normed(
                    both[:, :128], both[:, 128:], state, gain_ref[...]
                )

    return call(
        body,
        [jax.ShapeDtypeStruct((outs.shape[1], 256), BF16)],
        (second_core, outs, start, got, gain),
        (),
        1 << 28,
    )[0]


def finish_responses(flip, outs, outs_partner, ends, ends_partner, gain):
    parts = outs.shape[1] // 256

    def body(flip_ref, outs_ref, partner_ref, ends_ref, ends_partner_ref, gain_ref, *result_refs):
        for side, (source, states) in enumerate(
            ((outs_ref, ends_ref), (partner_ref, ends_partner_ref))
        ):
            base = (flip_ref[0] if side == 0 else 1 - flip_ref[0]) * 256
            for head in range(2):
                lanes = pl.ds(pl.multiple_of(base + head * 128, 128), 128)
                for part in range(parts):
                    both = source[head, pl.ds(part * 256, 256), :]
                    result_refs[part][:, lanes] = normed(
                        both[:, :128], both[:, 128:], states[head], gain_ref[...]
                    )

    return call(
        body,
        [jax.ShapeDtypeStruct((256, 512), BF16)] * parts,
        (flip, outs, outs_partner, ends, ends_partner, gain),
        (),
        1 << 29,
    )


def assemble(numbers, blocks):
    parts = len(blocks)

    def body(number_ref, *refs):
        result_ref = refs[parts]
        row = lax.broadcasted_iota(jnp.int32, (256, 512), 0)
        live = row < number_ref[1]
        for shift in range(parts):
            base = lax.rem(number_ref[0] + shift, parts) * 512
            block = refs[shift][...].astype(F32)
            result_ref[:, pl.ds(pl.multiple_of(base, 512), 512)] = jnp.where(
                live, block, 0.0
            ).astype(BF16)

    return call(body, [jax.ShapeDtypeStruct((256, 512 * parts), BF16)], (numbers, *blocks))[0]


def swap(array, axis):
    return lax.ppermute(array, axis, [(0, 1), (1, 0)])


def turn(array, axis, count, shift):
    return lax.ppermute(array, axis, [(i, (i + shift) % count) for i in range(count)])


def inner(
    prompt_tokens,
    response_tokens,
    w_query,
    w_key,
    w_value,
    w_decay,
    w_beta,
    decay_rate,
    beta_shift,
    out_gain,
    resp_lengths,
):
    core = lax.axis_index("core")
    along = lax.axis_index("x")
    side = lax.axis_index("y_hi")
    layer = lax.axis_index("z")
    upper = lax.axis_index("y_lo")
    layers = lax.axis_size("z")
    wide = lax.axis_size("x")
    tokens = response_tokens.reshape(response_tokens.shape[2:])
    token_parts = [tokens] + [turn(tokens, "x", wide, s) for s in range(1, wide)]

    rows = w_query.shape[0]
    gates_t = jnp.pad(jnp.concatenate([w_decay, w_beta], axis=1).T, ((0, 4), (0, 256 - rows)))
    pack_qk = jnp.concatenate([jnp.concatenate([w_query, w_key], axis=1), gates_t], axis=0)
    pack_v = jnp.concatenate([w_value, gates_t], axis=0)
    got = swap(jnp.where(core == 0, pack_v, pack_qk), "core")
    kept = jnp.where(core == 0, pack_qk, pack_v)
    low = jnp.where(core == 0, kept, got)
    high = jnp.where(core == 0, got, kept)
    mixed = jnp.concatenate(
        [low[rows:, :rows], high[rows:, :rows], jnp.zeros((8, 256 - 2 * rows), BF16)], axis=1
    )
    block = jnp.concatenate([low[:rows], high[:rows], mixed], axis=0)
    near = swap(block, "y_lo")
    pair = jnp.stack([jnp.where(upper == 0, block, near), jnp.where(upper == 0, near, block)])
    rising, falling, gathered = pair, pair, [pair]
    for step in range(layers // 2):
        rising = turn(rising, "z", layers, 1)
        gathered.append(rising)
        if step < layers // 2 - 1:
            falling = turn(falling, "z", layers, -1)
            gathered.append(falling)
    own = jnp.stack(gathered)
    other = swap(own, "core")

    def gates_of(group):
        return jnp.concatenate(
            [
                lax.dynamic_slice_in_dim(decay_rate, group * 2, 2),
                lax.dynamic_slice_in_dim(beta_shift, group * 2, 2),
            ]
        )

    core_number = core.reshape(1)
    spot = jnp.stack([core, layer])
    gain = out_gain.reshape(1, 128)
    group = along * 2 + side
    outs, mine, theirs = delta_rule(spot, gates_of(group), (prompt_tokens,), own, other, 8)
    first, chip_map = join_maps(core_number, mine, swap(theirs, "core"))
    first_chip, pair_map = join_chips(upper.reshape(1), chip_map, swap(chip_map, "y_lo"))
    pieces = [pair_map] + [turn(pair_map, "z", layers, s) for s in range(1, layers)]
    lent, _ = lax.optimization_barrier((own, pair_map))
    partner_own = swap(lent, "y_hi")
    (resp_outs,) = delta_rule(spot, gates_of(group), token_parts, own, other, 2)
    passed, _ = lax.optimization_barrier((partner_own, resp_outs))
    partner_other = swap(passed, "core")
    start, sent = run_prefix(
        jnp.stack([layer, upper, core]), pieces, first_chip, first, resp_outs
    )
    (resp_partner,) = delta_rule(
        spot, gates_of(along * 2 + 1 - side), token_parts, partner_own, partner_other, 2
    )
    got = swap(sent, "core")
    end_low = jnp.where(core == 0, sent[1], got[1])
    end_high = jnp.where(core == 0, got[1], sent[1])
    end_heads = jnp.stack([end_low, end_high])
    end_partner = swap(end_heads, "y_hi")
    parts = finish_responses(side.reshape(1), resp_outs, resp_partner, end_heads, end_partner, gain)
    blocks = [parts[0]] + [turn(parts[s], "x", wide, -s) for s in range(1, wide)]
    prompt_output = finish_prompt(core_number, outs, start, got, gain)
    numbers = jnp.stack([along, resp_lengths.reshape(())])
    result = assemble(numbers, blocks)
    return (prompt_output, result.reshape((1, 1) + result.shape))


def solution(mesh):
    devices = mesh.devices.reshape(mesh.shape["seq"] // 4, 2, 2, mesh.shape["grp"] // 2, 2)
    torus = Mesh(devices, ("z", "y_lo", "core", "x", "y_hi"))
    seq = ("z", "y_lo", "core")
    grp = ("x", "y_hi")
    weight = P(seq, grp)
    placed = (P(seq, None), P(grp, seq, None, None)) + (weight,) * 5 + (P(),) * 3 + (P(grp, seq),)
    return jax.shard_map(
        inner,
        mesh=torus,
        in_specs=placed,
        out_specs=(P(seq, grp), P(grp, seq, None, None)),
        check_vma=False,
    )
```

```python
import jax, jax.numpy as jnp
from jax import lax
from jax.sharding import Mesh
from jax.sharding import PartitionSpec as P
from jax.experimental import pallas as pl
from jax.experimental.pallas import tpu as pltpu


F32 = jnp.float32
BF16 = jnp.bfloat16
DK = 128
SPAN = 128
DEPTH = 2048
WIDTH = 8
VMEM = pl.BlockSpec(memory_space=pltpu.VMEM)
SMEM = pl.BlockSpec(memory_space=pltpu.SMEM)


def mm(a, b, ca=1, cb=0):
    return lax.dot_general(a, b, (((ca,), (cb,)), ((), ())), preferred_element_type=F32)


def halves(a):
    high = a.astype(BF16)
    return high, (a - high.astype(F32)).astype(BF16)


def mm_wide(a, b):
    a_high, a_low = halves(a)
    b_high, b_low = halves(b)
    a_both = jnp.concatenate([a_high, a_low], axis=1)
    return mm(a_both, jnp.concatenate([b_high, b_high], axis=0)) + mm(a_high, b_low)


def mm_low(a, b):
    return mm(a.astype(BF16), b.astype(BF16))


def mm_state(a, state):
    return mm(jnp.concatenate([a, a], axis=1), jnp.concatenate(halves(state), axis=0))


def unit_row(raw, scale):
    return (raw * (lax.rsqrt(jnp.sum(raw * raw, axis=-1, keepdims=True) + 1e-06) * scale)).astype(BF16)


def solve_units(lowers, row, column):
    ident = jnp.where(row == column, 1.0, 0.0).astype(F32)
    inside = (row // 8) == (column // 8)
    bases = [jnp.where(inside, lower, 0.0) for lower in lowers]
    squares = [mm_wide(base, base) for base in bases]
    fourths = [mm_wide(square, square) for square in squares]
    results = [ident - base for base in bases]
    results = [r + mm_wide(r, square) for r, square in zip(results, squares)]
    results = [r + mm_wide(r, fourth) for r, fourth in zip(results, fourths)]
    size = 8
    while size < SPAN:
        across = ((row // (2 * size)) == (column // (2 * size))) & (
            (row // size) != (column // size)
        )
        joined = [jnp.where(across, lower, 0.0).astype(BF16) for lower in lowers]
        rounded = [r.astype(BF16) for r in results]
        halfway = [mm(r, a).astype(BF16) for r, a in zip(rounded, joined)]
        results = [r - mm(h, b) for r, h, b in zip(results, halfway, rounded)]
        size *= 2
    return results


def make_body(chain, parts):
    def body(scalar_ref, gate_ref, x_refs, own_ref, other_ref, out_ref, map_ref, lent_ref,
             wqk_ref, wv_ref, wab_ref, q_ref, k_ref, v_ref, g_ref, b_ref,
             u_ref, lhs_ref, lhs2_ref, last_ref):
        second = scalar_ref[0]
        for block in range(16):
            rows = pl.ds(block * 128, 128)
            mine = own_ref[block // 2, block % 2]
            others = other_ref[block // 2, block % 2]
            first_half = jnp.where(second == 0, mine, others)
            second_half = jnp.where(second == 0, others, mine)
            wqk_ref[rows, :] = first_half[:128]
            wv_ref[rows, :] = second_half[:128]
            tall = jnp.concatenate(
                [first_half[128:136, :128].astype(F32), jnp.zeros((120, 128), F32)], axis=0
            )
            wab_ref[rows, :] = tall.T.astype(BF16)
        count = sum(x_ref.shape[0] for x_ref in x_refs)
        tril = jnp.where(
            lax.broadcasted_iota(jnp.int32, (SPAN, SPAN), 0)
            >= lax.broadcasted_iota(jnp.int32, (SPAN, SPAN), 1),
            1.0,
            0.0,
        ).astype(BF16)
        lane = lax.broadcasted_iota(jnp.int32, (1, 128), 1)
        rate = jnp.where(lane == 0, gate_ref[0], jnp.where(lane == 1, gate_ref[1], 0.0))
        shift = jnp.where(lane == 2, gate_ref[2], jnp.where(lane == 3, gate_ref[3], 0.0))
        for part in range(count // 256):
            rows = pl.ds(part * 256, 256)
            x = x_refs[part][...] if len(x_refs) > 1 else x_refs[0][rows, :]
            qk = mm(x, wqk_ref[...])
            q_ref[rows, :] = unit_row(qk[:, :128], DK ** (-0.5))
            k_ref[rows, :] = unit_row(qk[:, 128:], 1.0)
            v_ref[rows, :] = mm(x, wv_ref[...]).astype(BF16)
            ab = mm(x, wab_ref[...])
            g_ref[rows, :] = -rate * jnp.logaddexp(ab, 0.0)
            b_ref[rows, :] = 1.0 / (1.0 + jnp.exp(-(ab + shift)))
        row = lax.broadcasted_iota(jnp.int32, (SPAN, SPAN), 0)
        column = lax.broadcasted_iota(jnp.int32, (SPAN, SPAN), 1)
        spans = count // SPAN

        def prepare(index, carry):
            chains = [(sub, head) for sub in range(WIDTH) for head in range(2)]
            spans_now = [index * WIDTH + sub for sub in range(WIDTH)]
            rows = [pl.ds(pl.multiple_of(span * SPAN, SPAN), SPAN) for span in spans_now]
            q = [q_ref[r, :] for r in rows]
            k = [k_ref[r, :] for r in rows]
            beta = [b_ref[r, :] for r in rows]
            pieces = []
            for r in rows:
                g = g_ref[r, :]
                g_high, g_low = halves(g)
                pieces.append(
                    (g_high, g_low, (g - g_high.astype(F32) - g_low.astype(F32)).astype(BF16))
                )
            cumul = [
                mm(jnp.concatenate([tril, tril], axis=1), jnp.concatenate(p[:2], axis=0))
                + mm(tril, p[2])
                for p in pieces
            ]
            cumul_t = [c.T for c in cumul]
            kk = [mm(a, a, 1, 1) for a in k]
            qk = [mm(a, b, 1, 1) for a, b in zip(q, k)]
            col = [jnp.broadcast_to(cumul[s][:, h:h + 1], (SPAN, SPAN)) for s, h in chains]
            decay = [
                jnp.where(
                    row >= column, jnp.exp(jnp.minimum(c - cumul_t[s][h:h + 1, :], 0.0)), 0.0
                )
                for c, (s, h) in zip(col, chains)
            ]
            strength = [
                jnp.broadcast_to(beta[s][:, 2 + h:3 + h], (SPAN, SPAN)) for s, h in chains
            ]
            lowers = [
                jnp.where(row > column, b * d * kk[s], 0.0)
                for b, d, (s, h) in zip(strength, decay, chains)
            ]
            inverses = solve_units(lowers, row, column)
            solved = []
            for n, (s, h) in enumerate(chains):
                v = v_ref[rows[s], h * 128:(h + 1) * 128].astype(F32)
                rhs = jnp.concatenate(
                    [strength[n] * v, strength[n] * jnp.exp(col[n]) * k[s].astype(F32)], axis=1
                )
                solved.append(mm_low(inverses[n], rhs))
            for n, (s, h) in enumerate(chains):
                both = pl.ds(pl.multiple_of(spans_now[s] * 2 * SPAN, 2 * SPAN), 2 * SPAN)
                end = cumul[s][SPAN - 1:SPAN, h:h + 1]
                tail = jnp.exp(jnp.broadcast_to(end, (SPAN, SPAN)) - col[n]) * k[s].astype(F32)
                u_ref[h, rows[s], :] = solved[n][:, :128]
                lhs_ref[h, both, :] = jnp.concatenate(
                    [solved[n][:, 128:], jnp.exp(col[n]) * q[s].astype(F32)], axis=0
                ).astype(BF16)
                lhs2_ref[h, both, :] = jnp.concatenate(
                    [decay[n] * qk[s], tail.T], axis=0
                ).astype(BF16)
                last_ref[h, pl.ds(spans_now[s], 1), :] = jnp.broadcast_to(jnp.exp(end), (1, 128))
            return carry

        lax.fori_loop(0, spans // WIDTH, prepare, 0)
        ident = jnp.where(row == column, 1.0, 0.0).astype(F32)
        start = jnp.concatenate([jnp.zeros((128, 128), F32), ident], axis=1)
        lines = [(group, head) for group in range(spans // chain) for head in range(2)]
        states = [start for unused in lines]
        for step in range(chain):
            at = [group * chain + step for group, head in lines]
            reads = [
                mm_state(lhs_ref[head, pl.ds(span * 2 * SPAN, 2 * SPAN), :], state)
                for span, (group, head), state in zip(at, lines, states)
            ]
            deltas = [
                jnp.concatenate(
                    [u_ref[head, pl.ds(span * SPAN, SPAN), :] - r[:128, :128], -r[:128, 128:]],
                    axis=1,
                ).astype(BF16)
                for span, (group, head), r in zip(at, lines, reads)
            ]
            writes = [
                mm(lhs2_ref[head, pl.ds(span * 2 * SPAN, 2 * SPAN), :], delta)
                for span, (group, head), delta in zip(at, lines, deltas)
            ]
            lasts = [last_ref[head, pl.ds(span, 1), :] for span, (group, head) in zip(at, lines)]
            for span, (group, head), r, w in zip(at, lines, reads, writes):
                out_ref[head, pl.ds(span * SPAN, SPAN), :] = r[128:] + w[:128]
            states = [
                jnp.concatenate([last, last], axis=1) * state + w[128:]
                for last, state, w in zip(lasts, states, writes)
            ]
        if map_ref is not None:
            second_core = scalar_ref[0] == 1
            map_ref[...] = jnp.where(second_core, states[1], states[0])
            lent_ref[...] = jnp.where(second_core, states[0], states[1])

    def entry(scalar_ref, gate_ref, *refs):
        x_refs, refs = refs[:parts], refs[parts:]
        own_ref, other_ref, out_ref = refs[:3]
        if parts == 1:
            body(scalar_ref, gate_ref, x_refs, own_ref, other_ref, out_ref, *refs[3:])
        else:
            body(scalar_ref, gate_ref, x_refs, own_ref, other_ref, out_ref, None, None, *refs[3:])

    return entry


def delta_rule(second, gates, tokens, own, other, chain):
    count = sum(x.shape[0] for x in tokens)
    outs = [jax.ShapeDtypeStruct((2, count, 256), F32)]
    if len(tokens) == 1:
        outs += [jax.ShapeDtypeStruct((128, 256), F32)] * 2
    spans = count // SPAN
    return pl.pallas_call(
        make_body(chain, len(tokens)),
        out_shape=tuple(outs),
        in_specs=[SMEM, SMEM] + [VMEM] * (len(tokens) + 2),
        out_specs=tuple(VMEM for unused in outs),
        scratch_shapes=[
            pltpu.VMEM((DEPTH, 256), BF16),
            pltpu.VMEM((DEPTH, 256), BF16),
            pltpu.VMEM((DEPTH, 128), BF16),
            pltpu.VMEM((count, 128), BF16),
            pltpu.VMEM((count, 128), BF16),
            pltpu.VMEM((count, 256), BF16),
            pltpu.VMEM((count, 128), F32),
            pltpu.VMEM((count, 128), F32),
            pltpu.VMEM((2, count, 128), F32),
            pltpu.VMEM((2, 2 * count, 128), BF16),
            pltpu.VMEM((2, 2 * count, 128), BF16),
            pltpu.VMEM((2, max(spans, 8), 128), F32),
        ],
        cost_estimate=pl.CostEstimate(flops=2 * count * 2048 * 640 + 16 * 60 * 2 * 128**3, transcendentals=count * 1024, bytes_accessed=8 << 20),
        compiler_params=pltpu.CompilerParams(vmem_limit_bytes=48 << 20),
    )(second, gates, *tokens, own, other)


def call(body, outs, operands, scratch=(), flops=1 << 24):
    return pl.pallas_call(
        body,
        out_shape=tuple(outs),
        in_specs=[SMEM if a.ndim == 1 else VMEM for a in operands],
        out_specs=tuple(VMEM for unused in outs),
        scratch_shapes=list(scratch),
        cost_estimate=pl.CostEstimate(flops=flops, transcendentals=0, bytes_accessed=1 << 20),
        compiler_params=pltpu.CompilerParams(vmem_limit_bytes=48 << 20),
    )(*operands)


def identity():
    row = lax.broadcasted_iota(jnp.int32, (128, 128), 0)
    column = lax.broadcasted_iota(jnp.int32, (128, 128), 1)
    return jnp.where(row == column, 1.0, 0.0).astype(F32)


def join_maps(second_core, kept, got):
    def body(second_ref, kept_ref, got_ref, first_ref, chip_ref):
        second = second_ref[0]
        mine = kept_ref[...]
        others = got_ref[...]
        first = jnp.where(second == 0, mine, others)
        last = jnp.where(second == 0, others, mine)
        first_ref[...] = first
        joined = mm_wide(last[:, 128:], first)
        chip_ref[...] = jnp.concatenate(
            [joined[:, :128] + last[:, :128], joined[:, 128:] - identity()], axis=1
        ).astype(BF16)

    shape = (128, 256)
    return call(
        body,
        [jax.ShapeDtypeStruct(shape, F32), jax.ShapeDtypeStruct(shape, BF16)],
        (second_core, kept, got),
    )


def join_chips(upper, kept, got):
    def body(upper_ref, kept_ref, got_ref, first_ref, pair_ref):
        mine = kept_ref[...]
        others = got_ref[...]
        first = jnp.where(upper_ref[0] == 0, mine, others)
        last = jnp.where(upper_ref[0] == 0, others, mine)
        first_ref[...] = first
        joined = mm(last[:, 128:], first) + first.astype(F32) + last.astype(F32)
        pair_ref[...] = joined.astype(BF16)

    shape = jax.ShapeDtypeStruct((128, 256), BF16)
    return call(body, [shape, shape], (upper, kept, got))


def run_prefix(place, pieces, first_chip, first, after):
    pairs = len(pieces)

    def body(place_ref, *refs):
        piece_refs = refs[:pairs]
        chip_ref, first_ref, _, start_ref, send_ref, sorted_ref = refs[pairs:]
        me = place_ref[0]
        for shift in range(pairs):
            sorted_ref[lax.rem(me + pairs - shift, pairs)] = piece_refs[shift][...]
        state = jnp.zeros((128, 128), F32)
        for pair in range(pairs):
            @pl.when(me == pair)
            def store_start(state=state):
                start_ref[...] = state

            piece = sorted_ref[pair]
            state = state + mm_state(piece[:, 128:], state) + piece[:, :128].astype(F32)
        send_ref[1] = state
        chip = chip_ref[...]
        begin = start_ref[...]
        moved = begin + mm_state(chip[:, 128:], begin) + chip[:, :128].astype(F32)
        begin = jnp.where(place_ref[1] == 0, begin, moved)
        first = first_ref[...]
        later = mm_wide(first[:, 128:], begin) + first[:, :128]
        start_ref[...] = jnp.where(place_ref[2] == 0, begin, later)
        send_ref[0] = jnp.where(place_ref[2] == 0, later, begin)

    return pl.pallas_call(
        body,
        out_shape=(
            jax.ShapeDtypeStruct((128, 128), F32),
            jax.ShapeDtypeStruct((2, 128, 128), F32),
        ),
        in_specs=[SMEM] + [VMEM] * (pairs + 2) + [pl.BlockSpec(memory_space=pl.ANY)],
        out_specs=(VMEM, VMEM),
        scratch_shapes=[pltpu.VMEM((pairs, 128, 256), BF16)],
        cost_estimate=pl.CostEstimate(flops=1 << 27, transcendentals=0, bytes_accessed=1 << 20),
    )(place, *pieces, first_chip, first, after)


def normed(local, lifted, state, gain):
    total = local + mm_wide(lifted, state)
    mean = jnp.mean(total * total, axis=-1, keepdims=True)
    return (total * lax.rsqrt(mean + 1e-06) * gain).astype(BF16)


def finish_prompt(second_core, outs, start, got, gain):
    def body(second_ref, outs_ref, start_ref, got_ref, gain_ref, result_ref):
        mine = start_ref[...]
        others = got_ref[0]
        for head in range(2):
            state = jnp.where(second_ref[0] == head, mine, others)
            for part in range(outs.shape[1] // 256):
                rows = pl.ds(part * 256, 256)
                both = outs_ref[head, rows, :]
                result_ref[rows, head * 128:(head + 1) * 128] = normed(
                    both[:, :128], both[:, 128:], state, gain_ref[...]
                )

    return call(
        body,
        [jax.ShapeDtypeStruct((outs.shape[1], 256), BF16)],
        (second_core, outs, start, got, gain),
        (),
        1 << 28,
    )[0]


def finish_responses(flip, outs, outs_partner, ends, ends_partner, gain):
    parts = outs.shape[1] // 256

    def body(flip_ref, outs_ref, partner_ref, ends_ref, ends_partner_ref, gain_ref, *result_refs):
        for side, (source, states) in enumerate(
            ((outs_ref, ends_ref), (partner_ref, ends_partner_ref))
        ):
            base = (flip_ref[0] if side == 0 else 1 - flip_ref[0]) * 256
            for head in range(2):
                lanes = pl.ds(pl.multiple_of(base + head * 128, 128), 128)
                for part in range(parts):
                    both = source[head, pl.ds(part * 256, 256), :]
                    result_refs[part][:, lanes] = normed(
                        both[:, :128], both[:, 128:], states[head], gain_ref[...]
                    )

    return call(
        body,
        [jax.ShapeDtypeStruct((256, 512), BF16)] * parts,
        (flip, outs, outs_partner, ends, ends_partner, gain),
        (),
        1 << 29,
    )


def assemble(numbers, blocks):
    parts = len(blocks)

    def body(number_ref, *refs):
        result_ref = refs[parts]
        row = lax.broadcasted_iota(jnp.int32, (256, 512), 0)
        live = row < number_ref[1]
        for shift in range(parts):
            base = lax.rem(number_ref[0] + shift, parts) * 512
            block = refs[shift][...].astype(F32)
            result_ref[:, pl.ds(pl.multiple_of(base, 512), 512)] = jnp.where(
                live, block, 0.0
            ).astype(BF16)

    return call(body, [jax.ShapeDtypeStruct((256, 512 * parts), BF16)], (numbers, *blocks))[0]


def swap(array, axis):
    return lax.ppermute(array, axis, [(0, 1), (1, 0)])


def turn(array, axis, count, shift):
    return lax.ppermute(array, axis, [(i, (i + shift) % count) for i in range(count)])


def inner(
    prompt_tokens,
    response_tokens,
    w_query,
    w_key,
    w_value,
    w_decay,
    w_beta,
    decay_rate,
    beta_shift,
    out_gain,
    resp_lengths,
):
    core = lax.axis_index("core")
    along = lax.axis_index("x")
    side = lax.axis_index("y_hi")
    layer = lax.axis_index("z")
    upper = lax.axis_index("y_lo")
    layers = lax.axis_size("z")
    wide = lax.axis_size("x")
    tokens = response_tokens.reshape(response_tokens.shape[2:])
    token_parts = [tokens] + [turn(tokens, "x", wide, s) for s in range(1, wide)]

    rows = w_query.shape[0]
    gates_t = jnp.pad(jnp.concatenate([w_decay, w_beta], axis=1).T, ((0, 4), (0, 256 - rows)))
    pack_qk = jnp.concatenate([jnp.concatenate([w_query, w_key], axis=1), gates_t], axis=0)
    pack_v = jnp.concatenate([w_value, gates_t], axis=0)
    got = swap(jnp.where(core == 0, pack_v, pack_qk), "core")
    kept = jnp.where(core == 0, pack_qk, pack_v)
    low = jnp.where(core == 0, kept, got)
    high = jnp.where(core == 0, got, kept)
    mixed = jnp.concatenate(
        [low[rows:, :rows], high[rows:, :rows], jnp.zeros((8, 256 - 2 * rows), BF16)], axis=1
    )
    block = jnp.concatenate([low[:rows], high[:rows], mixed], axis=0)
    chips = layers * 2
    own = lax.all_to_all(
        jnp.broadcast_to(block[None], (chips,) + block.shape), ("z", "y_lo"), 0, 0, tiled=True
    )
    own = own.reshape((layers, 2) + block.shape)
    other = swap(own, "core")

    def gates_of(group):
        return jnp.concatenate(
            [
                lax.dynamic_slice_in_dim(decay_rate, group * 2, 2),
                lax.dynamic_slice_in_dim(beta_shift, group * 2, 2),
            ]
        )

    core_number = core.reshape(1)
    spot = jnp.stack([core, layer])
    gain = out_gain.reshape(1, 128)
    group = along * 2 + side
    outs, mine, theirs = delta_rule(spot, gates_of(group), (prompt_tokens,), own, other, 8)
    first, chip_map = join_maps(core_number, mine, swap(theirs, "core"))
    first_chip, pair_map = join_chips(upper.reshape(1), chip_map, swap(chip_map, "y_lo"))
    pieces = [pair_map] + [turn(pair_map, "z", layers, s) for s in range(1, layers)]
    lent, _ = lax.optimization_barrier((own, pair_map))
    partner_own = swap(lent, "y_hi")
    (resp_outs,) = delta_rule(spot, gates_of(group), token_parts, own, other, 2)
    passed, _ = lax.optimization_barrier((partner_own, resp_outs))
    partner_other = swap(passed, "core")
    start, sent = run_prefix(
        jnp.stack([layer, upper, core]), pieces, first_chip, first, resp_outs
    )
    (resp_partner,) = delta_rule(
        spot, gates_of(along * 2 + 1 - side), token_parts, partner_own, partner_other, 2
    )
    got = swap(sent, "core")
    end_low = jnp.where(core == 0, sent[1], got[1])
    end_high = jnp.where(core == 0, got[1], sent[1])
    end_heads = jnp.stack([end_low, end_high])
    end_partner = swap(end_heads, "y_hi")
    parts = finish_responses(side.reshape(1), resp_outs, resp_partner, end_heads, end_partner, gain)
    blocks = [parts[0]] + [turn(parts[s], "x", wide, -s) for s in range(1, wide)]
    prompt_output = finish_prompt(core_number, outs, start, got, gain)
    numbers = jnp.stack([along, resp_lengths.reshape(())])
    result = assemble(numbers, blocks)
    return (prompt_output, result.reshape((1, 1) + result.shape))


def solution(mesh):
    devices = mesh.devices.reshape(mesh.shape["seq"] // 4, 2, 2, mesh.shape["grp"] // 2, 2)
    torus = Mesh(devices, ("z", "y_lo", "core", "x", "y_hi"))
    seq = ("z", "y_lo", "core")
    grp = ("x", "y_hi")
    weight = P(seq, grp)
    placed = (P(seq, None), P(grp, seq, None, None)) + (weight,) * 5 + (P(),) * 3 + (P(grp, seq),)
    return jax.shard_map(
        inner,
        mesh=torus,
        in_specs=placed,
        out_specs=(P(seq, grp), P(grp, seq, None, None)),
        check_vma=False,
    )
```
